32 devices in a mesh: space: 16 (over z, x, core), chan: 2 (over y).
Axes of the slice: x: 2, y: 2, z: 4, core: 2. Of those that a mesh axis runs over, the one named last changes fastest.
Arguments:
- inputs: bfloat16 [64, 32, 64, 128], P('chan', 'space'), may hold values from -6 to 6
- grad_out: bfloat16 [64, 32, 64, 128], P('chan', 'space'), may hold values from -6 to 6
- filt: bfloat16 [27, 64, 64], P(None, 'chan'), may hold values from -0.15625 to 0.15625
Outputs:
- grad_inputs: bfloat16 [64, 32, 64, 128], P('chan', 'space')
- grad_filt: float32 [27, 64, 64], P(None, 'chan', 'space')
The draws below stay inside these ranges and needn't reach their ends.
All inputs are finite; a program needn't handle non-finite values.
Results may differ from the reference program's by a relative error of at most 0.0066.
Values may be sent and summed in bfloat16 or wider, within the bound.
No kernel may reach another device: no remote copies, remote signals or barrier semaphores. Data moves between devices by JAX's collectives and lax.ppermute only.
A program may use at most 128 MiB of HBM per device.

```python
import jax
import jax.numpy as jnp
from jax import lax

C = 64
O = 64
H = 64
W = 128
D = 32


def strengthened(entries, key, source, target, shards_of, factor):
    def block_of(position):
        return (jnp.arange(entries.shape[position]) // (entries.shape[position] // shards_of)).reshape((-1,) + (1,) * (entries.ndim - 1 - position))

    near = jax.random.permutation(key, shards_of)[block_of(target)]
    second = (block_of(target) + shards_of // 2) % shards_of
    return jnp.where((block_of(source) == near) | (block_of(source) == second), factor * entries, entries)


def steps_of(own_key, shape, cuts, low, largest):
    loudness, own = 1.0, jax.random.fold_in(own_key, 6)
    for dim, shards_of in cuts:
        heights = jnp.exp(jax.random.uniform(jax.random.fold_in(own, dim), (shards_of,), jnp.float32, low / len(cuts), largest / len(cuts)))
        loudness = loudness * jnp.repeat(heights, shape[dim] // shards_of).reshape([-1 if axis == dim else 1 for axis in range(len(shape))])
    return loudness


def noise(stream_key, extent, width, reach, pieces=(), kind=jnp.bfloat16):
    result = width * jax.random.normal(stream_key, extent, jnp.float32)
    if pieces:
        result = result * steps_of(stream_key, extent, pieces, -0.22, 0.18)
    return jnp.clip(result, -reach, reach).astype(kind)


def bell_draw_with(stream_key, dims, scale, bound, shards, heavy, dtype=jnp.bfloat16):
    array = scale * jax.random.normal(stream_key, dims, jnp.float32)
    if shards:
        array = array * steps_of(stream_key, dims, shards, -0.22, 0.18)
    return jnp.clip(strengthened(array, jax.random.fold_in(stream_key, 3), *heavy), -bound, bound).astype(dtype)


def setup_inputs(seed: int = 0) -> dict:
    splits = jax.random.split(jax.random.key(seed), 4)
    return {
        "inputs": noise(splits[0], (C, D, H, W), 1.0, 6.0, ((0, 2), (1, 16))),
        "grad_out": bell_draw_with(splits[1], (O, D, H, W), 1.0, 6.0, ((0, 2), (1, 16)), (1, 0, 16, 2.0)),
        "filt": noise(splits[2], (27, O, C), (27 * O) ** -0.5, 0.15625, ((1, 2),)),
    }


def reference(inputs, grad_out, filt):
    kernel = filt.astype(jnp.float32).reshape(3, 3, 3, O, C).transpose(3, 4, 0, 1, 2)

    def forward(volume, weights):
        return lax.conv_general_dilated(volume, weights, (1, 1, 1), [(1, 1), (1, 1), (1, 1)], dimension_numbers=('NCDHW', 'OIDHW', 'NCDHW'), precision=lax.Precision.HIGHEST)
    _, pullback = jax.vjp(forward, inputs.astype(jnp.float32)[None], kernel)
    grad_volume, grad_kernel = pullback(grad_out.astype(jnp.float32)[None])
    grad_inputs = grad_volume[0].astype(jnp.bfloat16)
    grad_filt = grad_kernel.transpose(2, 3, 4, 0, 1).reshape(27, O, C)
    return (grad_inputs, grad_filt)
```

```python
import functools

import jax
import jax.numpy as jnp
from jax import lax
from jax.experimental import pallas as pl
from jax.experimental.pallas import tpu as pltpu
from jax.sharding import PartitionSpec as P

ROWS = 4


def _round_up(x, m):
    return (x + m - 1) // m * m


def _conv_kernel(*refs, has_prev):
    main, before, after, inp, wgt = refs[:5]
    if has_prev:
        prev, gi, gf, s_ref, in_ref = refs[5:]
    else:
        gi, gf, s_ref, in_ref = refs[5:]
    planes, height, outs, width = main.shape
    chans = inp.shape[2]
    zero_s = jnp.zeros((planes + 2, 1, 3 * outs, width), s_ref.dtype)
    s_ref[:, 0:1] = zero_s
    s_ref[:, height + 1 : height + 2] = zero_s
    zero_i = jnp.zeros((planes, 1, chans, width), in_ref.dtype)
    in_ref[:, 0:1] = zero_i
    in_ref[:, height + 1 : height + 2] = zero_i
    in_ref[:, 1 : height + 1] = inp[...]
    lane = lax.broadcasted_iota(jnp.int32, (outs, width), 1)

    def shift(h, carry):
        for p in range(planes + 2):
            if p == 0:
                x = before[0, h]
            elif p == planes + 1:
                x = after[0, h]
            else:
                x = main[p - 1, h]
            xf = x.astype(jnp.float32)
            left = jnp.where(lane == width - 1, 0.0, pltpu.roll(xf, width - 1, 1))
            right = jnp.where(lane == 0, 0.0, pltpu.roll(xf, 1, 1))
            s_ref[p, h + 1, 0:outs, :] = left.astype(jnp.bfloat16)
            s_ref[p, h + 1, outs : 2 * outs, :] = x
            s_ref[p, h + 1, 2 * outs : 3 * outs, :] = right.astype(jnp.bfloat16)
        return carry

    lax.fori_loop(0, height, shift, 0)
    gf[...] = jnp.zeros(gf.shape, jnp.float32)

    def step(t, carry):
        h0 = t * ROWS
        for d in range(planes):
            cols = jnp.concatenate(
                [
                    jnp.concatenate(
                        [s_ref[d + j, h0 + q + i] for j in range(3) for i in range(3)], axis=0
                    )
                    for q in range(ROWS)
                ],
                axis=1,
            )
            y = jnp.dot(wgt[...], cols, preferred_element_type=jnp.float32)
            for q in range(ROWS):
                part = y[:, q * width : (q + 1) * width]
                if has_prev:
                    part = part + prev[d, h0 + q].astype(jnp.float32)
                gi[d, h0 + q] = part.astype(gi.dtype)
        left_side = jnp.concatenate(
            [
                jnp.concatenate([s_ref[d + j, h0 + q + 1] for j in range(3)], axis=0)
                for d in range(planes)
                for q in range(ROWS)
            ],
            axis=1,
        )
        right_side = jnp.concatenate(
            [
                jnp.concatenate([in_ref[d, h0 + q + b] for b in range(3)], axis=0)
                for d in range(planes)
                for q in range(ROWS)
            ],
            axis=1,
        )
        gf[...] += lax.dot_general(
            left_side,
            right_side,
            (((1,), (1,)), ((), ())),
            preferred_element_type=jnp.float32,
        )
        return carry

    lax.fori_loop(0, height // ROWS, step, 0)


def _conv(main, before, after, inp, wgt, prev, last):
    planes, height, outs, width = main.shape
    chans = inp.shape[2]
    args = [main, before, after, inp, wgt] + ([] if prev is None else [prev])
    vmem = pl.BlockSpec(memory_space=pltpu.VMEM)
    return pl.pallas_call(
        functools.partial(_conv_kernel, has_prev=prev is not None),
        in_specs=[vmem] * len(args),
        out_specs=[vmem, vmem],
        out_shape=[
            jax.ShapeDtypeStruct(
                (planes, height, chans, width), jnp.bfloat16 if last else jnp.float32
            ),
            jax.ShapeDtypeStruct((9 * outs, 3 * chans), jnp.float32),
        ],
        scratch_shapes=[
            pltpu.VMEM((planes + 2, height + 2, 3 * outs, width), jnp.bfloat16),
            pltpu.VMEM((planes, height + 2, chans, width), jnp.bfloat16),
        ],
        compiler_params=pltpu.CompilerParams(vmem_limit_bytes=56 * 1024 * 1024),
    )(*args)


def _pad_dim(x, dim, size):
    if x.shape[dim] == size:
        return x
    pads = [(0, 0)] * x.ndim
    pads[dim] = (0, size - x.shape[dim])
    return jnp.pad(x, pads)


def local(inputs, grad_out, filt):
    n = lax.axis_size("chan")
    s = lax.axis_size("space")
    me = lax.axis_index("chan")
    c_l, planes, height, width = inputs.shape
    o_l = grad_out.shape[0]
    c_all = filt.shape[2]
    cs = c_all // s
    per = c_l // cs
    o_p, c_p = _round_up(o_l, 16), _round_up(c_l, 16)
    up = [(i, i + 1) for i in range(s - 1)]
    down = [(j, i) for i, j in up]

    go = grad_out.transpose(1, 2, 0, 3)
    x = _pad_dim(inputs.transpose(1, 2, 0, 3), 2, c_p)
    own = [go[p : p + 1] for p in range(planes)]

    gi = None
    parts = []
    for r in range(n):
        rot = [((k + r) % n, k) for k in range(n)]
        block = lax.dynamic_slice_in_dim(filt, ((me - r) % n) * c_l, c_l, axis=2)
        if r:
            pieces = [lax.ppermute(v, "chan", rot) for v in own]
            block = lax.ppermute(block, "chan", rot)
        else:
            pieces = own
        after = lax.ppermute(pieces[0], "space", down)
        before = lax.ppermute(pieces[-1], "space", up)
        main = go if r == 0 else jnp.concatenate(pieces, axis=0)
        main, before, after = (_pad_dim(v, 2, o_p) for v in (main, before, after))
        wgt = block.reshape(3, 3, 3, o_l, c_l)[::-1, ::-1]
        wgt = _pad_dim(_pad_dim(wgt, 3, o_p), 4, c_p)
        wgt = wgt.transpose(4, 0, 1, 2, 3).reshape(c_p, 27 * o_p)
        gi, gf = _conv(main, before, after, x, wgt, gi, r == n - 1)
        gf = gf.reshape(3, 3, o_p, 3, c_p)[::-1, :, :o_l, :, :c_l]
        gf = gf.reshape(3, 3, o_l, 3, per, cs).transpose(4, 0, 3, 1, 2, 5)
        parts.append(gf.reshape(per, 27, o_l * cs))
    grad_inputs = gi[:, :, :c_l].transpose(2, 0, 1, 3)

    shares = jnp.concatenate(parts, axis=0)
    got = lax.all_to_all(shares, "space", 0, 0, tiled=True)
    mine = jnp.sum(got, axis=0)
    move = []
    for k in range(n):
        for i in range(s):
            r, cb = divmod(i, per)
            move.append((i * n + k, (k * per + cb) * n + (k + r) % n))
    mine = lax.ppermute(mine, ("space", "chan"), move)
    return (grad_inputs, mine.reshape(27, o_l, cs))


def solution(mesh):
    return jax.shard_map(
        local,
        mesh=mesh,
        in_specs=(
            P("chan", "space", None, None),
            P("chan", "space", None, None),
            P(None, "chan", None),
        ),
        out_specs=(P("chan", "space", None, None), P(None, "chan", "space")),
        check_vma=False,
    )
```

```python
import functools

import jax
import jax.numpy as jnp
from jax import lax
from jax.experimental import pallas as pl
from jax.experimental.pallas import tpu as pltpu
from jax.sharding import PartitionSpec as P

ROWS = 4


def _round_up(x, m):
    return (x + m - 1) // m * m


def _conv_kernel(*refs, planes, slot, step_c):
    field = refs[: planes + 2]
    inp, wgt = refs[planes + 2 : planes + 4]
    if slot:
        prev, prev_gf, gi, gf, s_ref, in_ref, acc = refs[planes + 4 :]
    else:
        gi, gf, s_ref, in_ref, acc = refs[planes + 4 :]
    height, outs, width = field[0].shape[1:]
    chans = inp.shape[2]
    groups = height // ROWS
    zero_s = jnp.zeros((planes + 2, 1, 3 * outs, width), s_ref.dtype)
    s_ref[:, 0:1] = zero_s
    s_ref[:, height + 1 : height + 2] = zero_s
    zero_i = jnp.zeros((planes, 1, chans, width), in_ref.dtype)
    in_ref[:, 0:1] = zero_i
    in_ref[:, height + 1 : height + 2] = zero_i
    acc[...] = jnp.zeros(acc.shape, jnp.float32)
    lane = lax.broadcasted_iota(jnp.int32, (outs, width), 1)

    def build(group):
        for q in range(ROWS):
            h = group * ROWS + q
            for p in range(planes + 2):
                x = field[p][0, h]
                xf = x.astype(jnp.float32)
                left = jnp.where(lane == width - 1, 0.0, pltpu.roll(xf, width - 1, 1))
                right = jnp.where(lane == 0, 0.0, pltpu.roll(xf, 1, 1))
                s_ref[p, h + 1, 0:outs, :] = left.astype(jnp.bfloat16)
                s_ref[p, h + 1, outs : 2 * outs, :] = x
                s_ref[p, h + 1, 2 * outs : 3 * outs, :] = right.astype(jnp.bfloat16)
            for d in range(planes):
                in_ref[d, h + 1] = inp[d, h]

    def multiply(group):
        h0 = group * ROWS
        for d in range(planes):
            cols = jnp.concatenate(
                [
                    jnp.concatenate(
                        [s_ref[d + j, h0 + q + i] for j in range(3) for i in range(3)], axis=0
                    )
                    for q in range(ROWS)
                ],
                axis=1,
            )
            y = jnp.dot(wgt[...], cols, preferred_element_type=jnp.float32)
            for q in range(ROWS):
                part = y[:, q * width : (q + 1) * width]
                if slot:
                    part = part + prev[d, h0 + q]
                gi[d, h0 + q] = part.astype(gi.dtype)
        out_side = jnp.concatenate(
            [
                jnp.concatenate([s_ref[d + j, h0 + q + 1] for j in range(3)], axis=0)
                for d in range(planes)
                for q in range(ROWS)
            ],
            axis=1,
        )
        in_side = jnp.concatenate(
            [
                jnp.concatenate([in_ref[d, h0 + q + b] for b in range(3)], axis=0)
                for d in range(planes)
                for q in range(ROWS)
            ],
            axis=1,
        )
        acc[...] += lax.dot_general(
            in_side, out_side, (((1,), (1,)), ((), ())), preferred_element_type=jnp.float32
        )

    build(0)
    build(1)

    def step(t, carry):
        multiply(t)
        build(t + 2)
        return carry

    lax.fori_loop(0, groups - 2, step, 0)
    multiply(groups - 2)
    multiply(groups - 1)
    own = gf.shape[0] // (slot + 1)
    if slot:
        gf[0 : slot * own] = prev_gf[...]
    for blk in range(own):
        for b in range(3):
            first = b * chans + blk * step_c
            gf[slot * own + blk, b * step_c : (b + 1) * step_c, :] = acc[first : first + step_c, :]


def _conv(field, inp, wgt, prev, slot, last, per, step_c):
    planes = len(field) - 2
    _, height, outs, width = field[0].shape
    chans = inp.shape[2]
    args = [*field, inp, wgt, *prev]
    vmem = pl.BlockSpec(memory_space=pltpu.VMEM)
    return pl.pallas_call(
        functools.partial(_conv_kernel, planes=planes, slot=slot, step_c=step_c),
        in_specs=[vmem] * len(args),
        out_specs=[vmem, vmem],
        out_shape=[
            jax.ShapeDtypeStruct(
                (planes, height, chans, width), jnp.bfloat16 if last else jnp.float32
            ),
            jax.ShapeDtypeStruct(((slot + 1) * per, 3 * step_c, 9 * outs), jnp.float32),
        ],
        scratch_shapes=[
            pltpu.VMEM((planes + 2, height + 2, 3 * outs, width), jnp.bfloat16),
            pltpu.VMEM((planes, height + 2, chans, width), jnp.bfloat16),
            pltpu.VMEM((3 * chans, 9 * outs), jnp.float32),
        ],
        compiler_params=pltpu.CompilerParams(vmem_limit_bytes=56 * 1024 * 1024),
    )(*args)


def _pad_dim(x, dim, size):
    if x.shape[dim] == size:
        return x
    pads = [(0, 0)] * x.ndim
    pads[dim] = (0, size - x.shape[dim])
    return jnp.pad(x, pads)


def local(inputs, grad_out, filt):
    n = lax.axis_size("chan")
    s = lax.axis_size("space")
    me = lax.axis_index("chan")
    c_l, planes, height, width = inputs.shape
    o_l = grad_out.shape[0]
    c_all = filt.shape[2]
    cs = c_all // s
    per = c_l // cs
    o_p, c_p = _round_up(o_l, 16), _round_up(c_l, 16)
    up = [(i, i + 1) for i in range(s - 1)]
    down = [(j, i) for i, j in up]

    own = [grad_out[:, p : p + 1].transpose(1, 2, 0, 3) for p in range(planes)]
    x = _pad_dim(inputs.transpose(1, 2, 0, 3), 2, c_p)

    rots = [[((k + r) % n, k) for k in range(n)] for r in range(n)]
    slots = [own] + [[lax.ppermute(v, "chan", rots[r]) for v in own] for r in range(1, n)]
    prev = ()
    for r in range(n):
        block = lax.dynamic_slice_in_dim(filt, ((me - r) % n) * c_l, c_l, axis=2)
        pieces = slots[r]
        if r:
            block = lax.ppermute(block, "chan", rots[r])
            if r == 1:
                pieces, prev = lax.optimization_barrier((pieces, prev))
        after = lax.ppermute(pieces[0], "space", down)
        before = lax.ppermute(pieces[-1], "space", up)
        field = [_pad_dim(v, 2, o_p) for v in (before, *pieces, after)]
        wgt = block.reshape(3, 3, 3, o_l, c_l)[::-1, ::-1]
        wgt = _pad_dim(_pad_dim(wgt, 3, o_p), 4, c_p)
        wgt = wgt.transpose(4, 0, 1, 2, 3).reshape(c_p, 27 * o_p)
        prev = _conv(field, x, wgt, prev, r, r == n - 1, per, cs)
    gi, shares = prev
    grad_inputs = gi[:, :, :c_l].transpose(2, 0, 1, 3)

    got = lax.all_to_all(shares, "space", 0, 0, tiled=True)
    mine = jnp.sum(got, axis=0)
    move = []
    for k in range(n):
        for i in range(s):
            r, cb = divmod(i, per)
            move.append((i * n + k, (k * per + cb) * n + (k + r) % n))
    mine = lax.ppermute(mine, ("space", "chan"), move)
    mine = mine.reshape(3, cs, 3, 3, o_p)[:, :, ::-1, :, :o_l]
    return (grad_inputs, mine.transpose(2, 0, 3, 4, 1).reshape(27, o_l, cs))


def solution(mesh):
    return jax.shard_map(
        local,
        mesh=mesh,
        in_specs=(
            P("chan", "space", None, None),
            P("chan", "space", None, None),
            P(None, "chan", None),
        ),
        out_specs=(P("chan", "space", None, None), P(None, "chan", "space")),
        check_vma=False,
    )
```

```python
import functools

import jax
import jax.numpy as jnp
from jax import lax
from jax.experimental import pallas as pl
from jax.experimental.pallas import tpu as pltpu
from jax.sharding import PartitionSpec as P

ROWS = 4


def _round_up(x, m):
    return (x + m - 1) // m * m


def _conv_kernel(*refs, count, taps, base, add, step_c):
    used = [d for d, pairs in enumerate(taps) if pairs]
    field, refs = refs[:count], refs[count:]
    weights, refs = dict(zip(used, refs)), refs[len(used) :]
    inp, refs = refs[0], refs[1:]
    has_prev = base > 0 or add
    if has_prev:
        prev, prev_gf, gi, gf, s_ref, in_ref, acc = refs
    else:
        gi, gf, s_ref, in_ref, acc = refs
    planes = len(taps)
    height, outs, width = field[0].shape[1:]
    chans = inp.shape[2]
    groups = height // ROWS
    zero_s = jnp.zeros((count, 1, 3 * outs, width), s_ref.dtype)
    s_ref[:, 0:1] = zero_s
    s_ref[:, height + 1 : height + 2] = zero_s
    zero_i = jnp.zeros((planes, 1, chans, width), in_ref.dtype)
    in_ref[:, 0:1] = zero_i
    in_ref[:, height + 1 : height + 2] = zero_i
    acc[...] = jnp.zeros(acc.shape, jnp.float32)
    lane = lax.broadcasted_iota(jnp.int32, (outs, width), 1)

    def build(group):
        for q in range(ROWS):
            h = group * ROWS + q
            for p in range(count):
                x = field[p][0, h]
                xf = x.astype(jnp.float32)
                left = jnp.where(lane == width - 1, 0.0, pltpu.roll(xf, width - 1, 1))
                right = jnp.where(lane == 0, 0.0, pltpu.roll(xf, 1, 1))
                s_ref[p, h + 1, 0:outs, :] = left.astype(jnp.bfloat16)
                s_ref[p, h + 1, outs : 2 * outs, :] = x
                s_ref[p, h + 1, 2 * outs : 3 * outs, :] = right.astype(jnp.bfloat16)
            for d in range(planes):
                in_ref[d, h + 1] = inp[d, h]

    def multiply(group):
        h0 = group * ROWS
        for d in range(planes):
            if not taps[d]:
                for q in range(ROWS):
                    gi[d, h0 + q] = prev[d, h0 + q].astype(gi.dtype)
                continue
            cols = jnp.concatenate(
                [
                    jnp.concatenate(
                        [s_ref[p, h0 + q + i] for p, _ in taps[d] for i in range(3)], axis=0
                    )
                    for q in range(ROWS)
                ],
                axis=1,
            )
            y = jnp.dot(weights[d][...], cols, preferred_element_type=jnp.float32)
            for q in range(ROWS):
                part = y[:, q * width : (q + 1) * width]
                if has_prev:
                    part = part + prev[d, h0 + q]
                gi[d, h0 + q] = part.astype(gi.dtype)
        for j in range(3):
            hits = [(d, p) for d in range(planes) for p, tap in taps[d] if tap == j]
            if not hits:
                continue
            out_side = jnp.concatenate(
                [s_ref[p, h0 + q + 1] for _, p in hits for q in range(ROWS)], axis=1
            )
            in_side = jnp.concatenate(
                [
                    jnp.concatenate([in_ref[d, h0 + q + b] for b in range(3)], axis=0)
                    for d, _ in hits
                    for q in range(ROWS)
                ],
                axis=1,
            )
            acc[j] += lax.dot_general(
                in_side, out_side, (((1,), (1,)), ((), ())), preferred_element_type=jnp.float32
            )

    build(0)
    build(1)

    def step(t, carry):
        multiply(t)
        build(t + 2)
        return carry

    lax.fori_loop(0, groups - 2, step, 0)
    multiply(groups - 2)
    multiply(groups - 1)
    own = gf.shape[0] // (base + 1)
    if base:
        gf[0 : base * own] = prev_gf[0 : base * own]
    for blk in range(own):
        for j in range(3):
            for b in range(3):
                first = b * chans + blk * step_c
                row = (j * 3 + b) * step_c
                value = acc[j, first : first + step_c, :]
                if add:
                    value = value + prev_gf[base * own + blk, row : row + step_c, :]
                gf[base * own + blk, row : row + step_c, :] = value


def _conv(field, inp, wgt, prev, taps, base, add, last, per, step_c):
    planes = len(taps)
    _, height, outs, width = field[0].shape
    chans = inp.shape[2]
    tap_len = 9 * outs
    weights = [
        jnp.concatenate([wgt[:, j * tap_len : (j + 1) * tap_len] for _, j in pairs], axis=1)
        for pairs in taps
        if pairs
    ]
    args = [*field, *weights, inp, *prev]
    vmem = pl.BlockSpec(memory_space=pltpu.VMEM)
    return pl.pallas_call(
        functools.partial(
            _conv_kernel, count=len(field), taps=taps, base=base, add=add, step_c=step_c
        ),
        in_specs=[vmem] * len(args),
        out_specs=[vmem, vmem],
        out_shape=[
            jax.ShapeDtypeStruct(
                (planes, height, chans, width), jnp.bfloat16 if last else jnp.float32
            ),
            jax.ShapeDtypeStruct(((base + 1) * per, 9 * step_c, 3 * outs), jnp.float32),
        ],
        scratch_shapes=[
            pltpu.VMEM((len(field), height + 2, 3 * outs, width), jnp.bfloat16),
            pltpu.VMEM((planes, height + 2, chans, width), jnp.bfloat16),
            pltpu.VMEM((3, 3 * chans, 3 * outs), jnp.float32),
        ],
        compiler_params=pltpu.CompilerParams(vmem_limit_bytes=56 * 1024 * 1024),
    )(*args)


def _pad_dim(x, dim, size):
    if x.shape[dim] == size:
        return x
    pads = [(0, 0)] * x.ndim
    pads[dim] = (0, size - x.shape[dim])
    return jnp.pad(x, pads)


def local(inputs, grad_out, filt):
    n = lax.axis_size("chan")
    s = lax.axis_size("space")
    me = lax.axis_index("chan")
    c_l, planes, height, width = inputs.shape
    o_l = grad_out.shape[0]
    c_all = filt.shape[2]
    cs = c_all // s
    per = c_l // cs
    o_p, c_p = _round_up(o_l, 16), _round_up(c_l, 16)
    up = [(i, i + 1) for i in range(s - 1)]
    down = [(j, i) for i, j in up]

    own = [grad_out[:, p : p + 1].transpose(1, 2, 0, 3) for p in range(planes)]
    x = _pad_dim(inputs.transpose(1, 2, 0, 3), 2, c_p)

    rots = [[((k + r) % n, k) for k in range(n)] for r in range(n)]
    slots = [own] + [[lax.ppermute(v, "chan", rots[r]) for v in own] for r in range(1, n)]
    every = [[(d + j, j) for j in range(3)] for d in range(planes)]
    near = [[(d + j - 1, j) for j in range(3) if 0 <= d + j - 1 < planes] for d in range(planes)]
    far = [[] for _ in range(planes)]
    far[0].append((0, 0))
    far[-1].append((1, 2))
    prev = ()
    for r in range(n):
        block = lax.dynamic_slice_in_dim(filt, ((me - r) % n) * c_l, c_l, axis=2)
        pieces = slots[r]
        if r:
            block = lax.ppermute(block, "chan", rots[r])
            if r == 1:
                pieces, block, prev = lax.optimization_barrier((pieces, block, prev))
        after = lax.ppermute(pieces[0], "space", down)
        before = lax.ppermute(pieces[-1], "space", up)
        inner = [_pad_dim(v, 2, o_p) for v in pieces]
        outer = [_pad_dim(v, 2, o_p) for v in (before, after)]
        wgt = block.reshape(3, 3, 3, o_l, c_l)[::-1, ::-1]
        wgt = _pad_dim(_pad_dim(wgt, 3, o_p), 4, c_p)
        wgt = wgt.transpose(4, 0, 1, 2, 3).reshape(c_p, 27 * o_p)
        last = r == n - 1
        if r == 0:
            field = [outer[0], *inner, outer[1]]
            prev = _conv(field, x, wgt, prev, every, r, False, last, per, cs)
        else:
            prev = _conv(inner, x, wgt, prev, near, r, False, False, per, cs)
            prev = _conv(outer, x, wgt, prev, far, r, True, last, per, cs)
    gi, shares = prev
    grad_inputs = gi[:, :, :c_l].transpose(2, 0, 1, 3)

    got = lax.all_to_all(shares, "space", 0, 0, tiled=True)
    mine = jnp.sum(got, axis=0)
    move = []
    for k in range(n):
        for i in range(s):
            r, cb = divmod(i, per)
            move.append((i * n + k, (k * per + cb) * n + (k + r) % n))
    mine = lax.ppermute(mine, ("space", "chan"), move)
    mine = mine.reshape(3, 3, cs, 3, o_p)[::-1, :, :, :, :o_l]
    return (grad_inputs, mine.transpose(0, 1, 3, 4, 2).reshape(27, o_l, cs))


def solution(mesh):
    return jax.shard_map(
        local,
        mesh=mesh,
        in_specs=(
            P("chan", "space", None, None),
            P("chan", "space", None, None),
            P(None, "chan", None),
        ),
        out_specs=(P("chan", "space", None, None), P(None, "chan", "space")),
        check_vma=False,
    )
```
